512 devices in a mesh: rep: 2 (over y), blk: 128 (over z, x), head: 2 (over core).
Axes of the slice: x: 8, y: 2, z: 16, core: 2. Of those that a mesh axis runs over, the one named last changes fastest.
The devices are a block of a 8x16x16 slice.
Arguments:
- queries: bfloat16 [2, 8192, 8192], P('rep', 'blk', 'head'), parts along dimension 0, may hold values from -200 to 200
- keys: bfloat16 [2, 8192, 512], P('rep', 'blk', 'head'), parts along dimension 0, may hold values from -6 to 6
- values: bfloat16 [2, 8192, 512], P('rep', 'blk', 'head'), parts along dimension 0, may hold values from -6 to 6
- prompt_length: int32 [2], P('rep'), parts along dimension 0, may hold values from 4096 to 8192
- span_order: int32 [512], P('rep'), parts along dimension 0, may hold values from 0 to 255, as said below
Outputs:
- attended: bfloat16 [2, 8192, 8192], P('rep', 'blk', 'head'), parts along dimension 0
The draws below stay inside these ranges and needn't reach their ends.
There are 2 independent parts, one for each index of `rep`. The reference program is written for one: setup_inputs(seed, part) draws one part's arguments, and reference() takes and returns one part's arrays. A program takes and returns all parts, laid end to end along the dimension named above; each array names one. Nothing has to cross between parts.
Inputs may be any that keep to these rules, and one draw needn't show every extreme that they name: `span_order`: each of the 256 span numbers stands in exactly one slot.
All inputs are finite; a program needn't handle non-finite values.
Results may differ from the reference program's by a relative error of at most 0.0065.
Values may be sent and summed in bfloat16 or wider, within the bound.
No kernel may reach another device: no remote copies, remote signals or barrier semaphores. Data moves between devices by JAX's collectives and lax.ppermute only.
A program may use at most 64 MiB of HBM per device.

```python
import jax
import jax.numpy as jnp
from jax import lax

CH = 32
REPLICA_PROMPTS = 1
KEY_VALUE_HEADS = 4
QUERY_PER_KV = 16
HEAD_WIDTH = 128
NCHUNK = 256
PROMPT_TOKENS = 8192


def span_table(key):
    return jax.random.permutation(jax.random.fold_in(key, 11), NCHUNK).astype(jnp.int32)


def draw_span_order(key, part):
    return span_table(key)


def base_keys(key):
    unscaled_scores = jax.random.normal(jax.random.fold_in(key, 23), (REPLICA_PROMPTS, PROMPT_TOKENS, KEY_VALUE_HEADS, HEAD_WIDTH), jnp.float32)
    return jnp.clip(unscaled_scores, -6.0, 6.0)


def draw_keys(key, part):
    unscaled_scores = base_keys(key)
    return unscaled_scores.reshape(REPLICA_PROMPTS, PROMPT_TOKENS, KEY_VALUE_HEADS * HEAD_WIDTH).astype(jnp.bfloat16)


def draw_queries(key, part):
    unscaled_scores = jax.random.normal(jax.random.fold_in(key, 31), (REPLICA_PROMPTS, PROMPT_TOKENS, KEY_VALUE_HEADS, QUERY_PER_KV, HEAD_WIDTH), jnp.float32)
    unscaled_scores = jnp.clip(unscaled_scores, -6.0, 6.0)
    return unscaled_scores.reshape(REPLICA_PROMPTS, PROMPT_TOKENS, KEY_VALUE_HEADS * QUERY_PER_KV * HEAD_WIDTH).astype(jnp.bfloat16)


def block_levels(key, dims, cuts, low, high):
    gain, own = 1.0, jax.random.fold_in(key, 6)
    for dim, shards_of in cuts:
        draws = jnp.exp(jax.random.uniform(jax.random.fold_in(own, dim), (shards_of,), jnp.float32, low / len(cuts), high / len(cuts)))
        gain = gain * jnp.repeat(draws, dims[dim] // shards_of).reshape([-1 if axis == dim else 1 for axis in range(len(dims))])
    return gain


def normal_values(key, shape, width, bound, pieces=(), held_as=jnp.bfloat16):
    entries = jax.random.normal(key, shape, jnp.float32) * width
    if len(pieces) > 0:
        entries = block_levels(key, shape, pieces, -0.22, 0.18) * entries
    return jnp.clip(entries, min=-bound, max=bound).astype(held_as)


def setup_inputs(seed: int = 0, part: int = 0) -> dict:
    key_list = jax.random.split(jax.random.key(seed), 6)
    part_splits = jax.random.split(jax.random.fold_in(key_list[5], part), 6)
    queries = draw_queries(jax.random.fold_in(jax.random.fold_in(key_list[5], part), 71), part)
    keys = draw_keys(jax.random.fold_in(jax.random.fold_in(key_list[5], part), 71), part)
    values = normal_values(part_splits[2], (REPLICA_PROMPTS, PROMPT_TOKENS, KEY_VALUE_HEADS * HEAD_WIDTH), 1.0, 6.0, ((1, 128), (2, 2)))
    prompt_length = jax.random.randint(part_splits[3], (REPLICA_PROMPTS,), PROMPT_TOKENS // 2, PROMPT_TOKENS + 1).astype(jnp.int32)
    span_order = draw_span_order(jax.random.fold_in(jax.random.fold_in(key_list[5], part), 71), part)
    return {"queries": queries, "keys": keys, "values": values, "prompt_length": prompt_length, "span_order": span_order}


NEG_FILL = -1e30


def one_prompt(queries, keys, values, limit, position):
    allowed = (position[None, :] <= position[:, None]) & (position[None, :] < limit)
    query_heads = queries.reshape(PROMPT_TOKENS, KEY_VALUE_HEADS, QUERY_PER_KV, HEAD_WIDTH).transpose(1, 2, 0, 3).reshape(KEY_VALUE_HEADS * QUERY_PER_KV, PROMPT_TOKENS, HEAD_WIDTH)
    key_heads = jnp.repeat(keys.reshape(PROMPT_TOKENS, KEY_VALUE_HEADS, HEAD_WIDTH).transpose(1, 0, 2), QUERY_PER_KV, axis=0)
    value_heads = jnp.repeat(values.reshape(PROMPT_TOKENS, KEY_VALUE_HEADS, HEAD_WIDTH).transpose(1, 0, 2), QUERY_PER_KV, axis=0)
    scale = HEAD_WIDTH ** -0.5

    def one_head(parts):
        query, key_rows, value_rows = parts
        scores = jnp.dot(query, key_rows.T, preferred_element_type=jnp.float32) * scale
        scores = jnp.where(allowed, scores, NEG_FILL)
        top = jnp.max(scores, axis=1, keepdims=True)
        weights = jnp.where(allowed, jnp.exp(scores - top), 0.0)
        total = jnp.sum(weights, axis=1, keepdims=True)
        mixed = jnp.dot(weights.astype(jnp.bfloat16), value_rows, preferred_element_type=jnp.float32)
        return mixed / total

    head_results = lax.map(one_head, (query_heads, key_heads, value_heads))
    joined_heads = head_results.reshape(KEY_VALUE_HEADS, QUERY_PER_KV, PROMPT_TOKENS, HEAD_WIDTH).transpose(2, 0, 1, 3).reshape(PROMPT_TOKENS, KEY_VALUE_HEADS * QUERY_PER_KV * HEAD_WIDTH)
    joined_heads = jnp.where((position < limit)[:, None], joined_heads, 0.0)
    return joined_heads.astype(jnp.bfloat16)


def reference(queries, keys, values, prompt_length, span_order):
    offsets = jnp.arange(CH, dtype=jnp.int32)
    position = (span_order[:, None].astype(jnp.int32) * CH + offsets[None, :]).reshape(-1).astype(jnp.int32)
    outputs = []
    for index in range(REPLICA_PROMPTS):
        outputs.append(one_prompt(queries[index], keys[index], values[index], prompt_length[index], position))
    return jnp.stack(outputs)
```

```python
import jax
import jax.numpy as jnp
from jax import lax
from jax.experimental import pallas as pl
from jax.experimental.pallas import tpu as pltpu
from jax.sharding import Mesh
from jax.sharding import PartitionSpec as P

HEAD_WIDTH = 128
BLK = ("blk_0", "blk_1")
BLOCK_SPANS = 16
NEG_FILL = -1e30
LOG2_E = 1.4426950408889634


def attend(table, q, gathered, local_heads, group, span):
    devices = gathered.shape[0]
    spans = devices * 2
    blocks = spans // BLOCK_SPANS
    keys_of = BLOCK_SPANS * span
    rows = group * span
    factor = LOG2_E * HEAD_WIDTH ** (-0.5)

    def kernel(table_ref, q_ref, kv_hbm, o_ref, kv_buf, s_buf, q_buf, m_buf, acc_buf, sems):
        limit = table_ref[spans + 2]

        def blocks_of(which):
            place = table_ref[spans + which]
            return jnp.where(place * span < limit, place // BLOCK_SPANS + 1, 0)

        most = jnp.maximum(blocks_of(0), blocks_of(1))

        def fetch(b, _):
            for i in range(BLOCK_SPANS):
                place = b * BLOCK_SPANS + i
                slot = table_ref[place]
                pltpu.make_async_copy(
                    kv_hbm.at[slot // 2, :, pl.ds(pl.multiple_of((slot % 2) * span, span), span), :],
                    kv_buf.at[:, pl.ds(pl.multiple_of(place * span, span), span), :],
                    sems.at[b],
                ).start()
            return 0

        lax.fori_loop(0, most, fetch, 0)

        def arrived(b):
            part = kv_buf.at[:, pl.ds(pl.multiple_of(b * keys_of, keys_of), keys_of), :]
            pltpu.make_async_copy(part, part, sems.at[b]).wait()

        def tile(t, _):
            head = t // 2
            which = t % 2
            place = table_ref[spans + which]
            count = blocks_of(which)
            row0 = pl.multiple_of(which * span, span)
            fresh = jnp.where(which == 0, 0, blocks_of(0))

            def columns(g):
                return pl.ds(pl.multiple_of((head * group + g) * HEAD_WIDTH, HEAD_WIDTH), HEAD_WIDTH)

            @pl.when(count == 0)
            def _():
                for g in range(group):
                    o_ref[pl.ds(row0, span), columns(g)] = jnp.zeros((span, HEAD_WIDTH), o_ref.dtype)

            @pl.when(count > 0)
            def _():
                for g in range(group):
                    q_buf[g * span : (g + 1) * span, :] = q_ref[pl.ds(row0, span), columns(g)]
                m_buf[...] = jnp.full(m_buf.shape, NEG_FILL, jnp.float32)
                acc_buf[...] = jnp.zeros(acc_buf.shape, jnp.float32)

                def score(b, masked):
                    @pl.when((head == 0) & (b >= fresh))
                    def _():
                        arrived(b)

                    part = kv_buf[head, pl.ds(pl.multiple_of(b * keys_of, keys_of), keys_of), :]
                    s = lax.dot_general(
                        q_buf[...], part, (((1,), (1,)), ((), ())), preferred_element_type=jnp.float32
                    )
                    if masked:
                        key_pos = b * keys_of + lax.broadcasted_iota(jnp.int32, s.shape, 1)
                        row_pos = place * span + lax.broadcasted_iota(jnp.int32, s.shape, 0) % span
                        s = jnp.where(key_pos <= row_pos, s, NEG_FILL)
                    s_buf[b] = s
                    top = m_buf[...]
                    for c in range(keys_of // 128):
                        top = jnp.maximum(top, s[:, c * 128 : (c + 1) * 128])
                    m_buf[...] = top

                def plain(b, _):
                    score(b, False)
                    return 0

                lax.fori_loop(0, count - 1, plain, 0)
                score(count - 1, True)
                m_buf[...] = jnp.broadcast_to(jnp.max(m_buf[...], axis=1, keepdims=True), m_buf.shape)

                def mix(b, _):
                    top = jnp.concatenate([m_buf[...]] * (keys_of // 128), axis=1)
                    w = jnp.exp2((s_buf[b] - top) * factor).astype(jnp.bfloat16)
                    v = kv_buf[local_heads + head, pl.ds(pl.multiple_of(b * keys_of, keys_of), keys_of), :]
                    wide = jnp.concatenate([v, jnp.ones_like(v)], axis=1)
                    acc_buf[...] += jnp.dot(w, wide, preferred_element_type=jnp.float32)
                    return 0

                lax.fori_loop(0, count, mix, 0)
                out = acc_buf[:, :HEAD_WIDTH] / acc_buf[:, HEAD_WIDTH:]
                row_pos = place * span + lax.broadcasted_iota(jnp.int32, out.shape, 0) % span
                out = jnp.where(row_pos < limit, out, 0.0).astype(o_ref.dtype)
                for g in range(group):
                    o_ref[pl.ds(row0, span), columns(g)] = out[g * span : (g + 1) * span]

            return 0

        lax.fori_loop(0, 2 * local_heads, tile, 0)

    return pl.pallas_call(
        kernel,
        out_shape=jax.ShapeDtypeStruct(q.shape, q.dtype),
        in_specs=[
            pl.BlockSpec(memory_space=pltpu.SMEM),
            pl.BlockSpec(memory_space=pltpu.VMEM),
            pl.BlockSpec(memory_space=pl.ANY),
        ],
        out_specs=pl.BlockSpec(memory_space=pltpu.VMEM),
        scratch_shapes=[
            pltpu.VMEM((2 * local_heads, spans * span, HEAD_WIDTH), jnp.bfloat16),
            pltpu.VMEM((blocks, rows, keys_of), jnp.float32),
            pltpu.VMEM((rows, HEAD_WIDTH), jnp.bfloat16),
            pltpu.VMEM((rows, 128), jnp.float32),
            pltpu.VMEM((rows, 2 * HEAD_WIDTH), jnp.float32),
            pltpu.SemaphoreType.DMA((blocks,)),
        ],
        compiler_params=pltpu.CompilerParams(vmem_limit_bytes=48 * 1024 * 1024),
    )(table, q, gathered)


def shards(queries, keys, values, prompt_length, span_order):
    mine = lax.axis_index(BLK)
    tok_rows = queries.shape[1]
    span = tok_rows // 2
    local_heads = keys.shape[2] // HEAD_WIDTH
    group = queries.shape[2] // (local_heads * HEAD_WIDTH)
    spans = span_order.shape[0]
    every = jnp.arange(spans, dtype=jnp.int32)
    slot_of = jnp.sum(jnp.where(span_order[None, :] == every[:, None], every[None, :], 0), axis=1)
    table = jnp.concatenate(
        [slot_of, lax.dynamic_slice_in_dim(span_order, mine * 2, 2), prompt_length]
    ).astype(jnp.int32)
    pieces = [keys[0, :, h * HEAD_WIDTH : (h + 1) * HEAD_WIDTH] for h in range(local_heads)]
    pieces += [values[0, :, h * HEAD_WIDTH : (h + 1) * HEAD_WIDTH] for h in range(local_heads)]
    packed = jnp.stack(pieces)
    gathered = lax.all_gather(packed, BLK, axis=0, tiled=False)
    return attend(table, queries[0], gathered, local_heads, group, span)[None]


def solution(mesh):
    blk = mesh.shape["blk"]
    split = Mesh(
        mesh.devices.reshape(mesh.shape["rep"], blk // 8, 8, mesh.shape["head"]),
        ("rep", "blk_0", "blk_1", "head"),
    )
    in_specs = (
        P("rep", BLK, "head"),
        P("rep", BLK, "head"),
        P("rep", BLK, "head"),
        P("rep"),
        P("rep"),
    )
    out_specs = P("rep", BLK, "head")
    return jax.shard_map(
        shards, mesh=split, in_specs=in_specs, out_specs=out_specs, check_vma=False
    )
```

```python
import jax
import jax.numpy as jnp
from jax import lax
from jax.experimental import pallas as pl
from jax.experimental.pallas import tpu as pltpu
from jax.sharding import Mesh
from jax.sharding import PartitionSpec as P

HEAD_WIDTH = 128
BLK = ("blk_0", "blk_1")
BLOCK_SPANS = 16
NEG_FILL = -1e30
LOG2_E = 1.4426950408889634
SENT_SCALE = 4096.0


def attend(table, q, gathered, group, span):
    columns_of, rows_of = gathered.shape[:2]
    spans = columns_of * rows_of * 2
    blocks = spans // BLOCK_SPANS
    keys_of = BLOCK_SPANS * span
    rows = group * span
    factor = LOG2_E * HEAD_WIDTH ** (-0.5) / SENT_SCALE

    def kernel(table_ref, q_ref, kv_hbm, o_ref, kv_buf, s_buf, q_buf, m_buf, acc_buf, sems):
        limit = table_ref[spans + 2]

        def blocks_of(which):
            place = table_ref[spans + which]
            return jnp.where(place * span < limit, place // BLOCK_SPANS + 1, 0)

        most = jnp.maximum(blocks_of(0), blocks_of(1))

        def fetch(b, _):
            for i in range(BLOCK_SPANS):
                place = b * BLOCK_SPANS + i
                slot = table_ref[place]
                pltpu.make_async_copy(
                    kv_hbm.at[
                        (slot // 2) % columns_of,
                        slot // (2 * columns_of),
                        :,
                        pl.ds(pl.multiple_of((slot % 2) * span, span), span),
                        :,
                    ],
                    kv_buf.at[:, pl.ds(pl.multiple_of(place * span, span), span), :],
                    sems.at[b],
                ).start()
            return 0

        lax.fori_loop(0, most, fetch, 0)

        def arrived(b):
            part = kv_buf.at[:, pl.ds(pl.multiple_of(b * keys_of, keys_of), keys_of), :]
            pltpu.make_async_copy(part, part, sems.at[b]).wait()

        def tile(which, _):
            place = table_ref[spans + which]
            count = blocks_of(which)
            row0 = pl.multiple_of(which * span, span)
            fresh = jnp.where(which == 0, 0, blocks_of(0))

            def columns(g):
                return pl.ds(g * HEAD_WIDTH, HEAD_WIDTH)

            @pl.when(count == 0)
            def _():
                for g in range(group):
                    o_ref[pl.ds(row0, span), columns(g)] = jnp.zeros((span, HEAD_WIDTH), o_ref.dtype)

            @pl.when(count > 0)
            def _():
                for g in range(group):
                    q_buf[g * span : (g + 1) * span, :] = q_ref[pl.ds(row0, span), columns(g)]
                m_buf[...] = jnp.full(m_buf.shape, NEG_FILL, jnp.float32)
                acc_buf[...] = jnp.zeros(acc_buf.shape, jnp.float32)

                def score(b, masked):
                    @pl.when(b >= fresh)
                    def _():
                        arrived(b)

                    part = kv_buf[0, pl.ds(pl.multiple_of(b * keys_of, keys_of), keys_of), :]
                    s = lax.dot_general(
                        q_buf[...], part, (((1,), (1,)), ((), ())), preferred_element_type=jnp.float32
                    )
                    if masked:
                        key_pos = b * keys_of + lax.broadcasted_iota(jnp.int32, s.shape, 1)
                        row_pos = place * span + lax.broadcasted_iota(jnp.int32, s.shape, 0) % span
                        s = jnp.where(key_pos <= row_pos, s, NEG_FILL)
                    s_buf[b] = s
                    top = m_buf[...]
                    for c in range(keys_of // 128):
                        top = jnp.maximum(top, s[:, c * 128 : (c + 1) * 128])
                    m_buf[...] = top

                def plain(b, _):
                    score(b, False)
                    return 0

                lax.fori_loop(0, count - 1, plain, 0)
                score(count - 1, True)
                m_buf[...] = jnp.broadcast_to(jnp.max(m_buf[...], axis=1, keepdims=True), m_buf.shape)

                def mix(b, _):
                    top = jnp.concatenate([m_buf[...]] * (keys_of // 128), axis=1)
                    w = jnp.exp2((s_buf[b] - top) * factor).astype(jnp.bfloat16)
                    v = kv_buf[1, pl.ds(pl.multiple_of(b * keys_of, keys_of), keys_of), :]
                    wide = jnp.concatenate([v, jnp.ones_like(v)], axis=1)
                    acc_buf[...] += jnp.dot(w, wide, preferred_element_type=jnp.float32)
                    return 0

                lax.fori_loop(0, count, mix, 0)
                out = acc_buf[:, :HEAD_WIDTH] / (acc_buf[:, HEAD_WIDTH:] * SENT_SCALE)
                row_pos = place * span + lax.broadcasted_iota(jnp.int32, out.shape, 0) % span
                out = jnp.where(row_pos < limit, out, 0.0).astype(o_ref.dtype)
                for g in range(group):
                    o_ref[pl.ds(row0, span), columns(g)] = out[g * span : (g + 1) * span]

            return 0

        lax.fori_loop(0, 2, tile, 0)

    return pl.pallas_call(
        kernel,
        out_shape=jax.ShapeDtypeStruct(q.shape, q.dtype),
        in_specs=[
            pl.BlockSpec(memory_space=pltpu.SMEM),
            pl.BlockSpec(memory_space=pltpu.VMEM),
            pl.BlockSpec(memory_space=pl.ANY),
        ],
        out_specs=pl.BlockSpec(memory_space=pltpu.VMEM),
        scratch_shapes=[
            pltpu.VMEM((2, spans * span, HEAD_WIDTH), jnp.bfloat16),
            pltpu.VMEM((blocks, rows, keys_of), jnp.float32),
            pltpu.VMEM((rows, HEAD_WIDTH), jnp.bfloat16),
            pltpu.VMEM((rows, 128), jnp.float32),
            pltpu.VMEM((rows, 2 * HEAD_WIDTH), jnp.float32),
            pltpu.SemaphoreType.DMA((blocks,)),
        ],
        compiler_params=pltpu.CompilerParams(vmem_limit_bytes=40 * 1024 * 1024),
    )(table, q, gathered)


def shards(queries, keys, values, prompt_length, span_order):
    mine = lax.axis_index(BLK)
    lines = lax.axis_size("blk_1")
    half = lax.axis_index("blk_0") % 2
    partner = mine + (1 - 2 * half) * lines
    tok_rows = queries.shape[1]
    span = tok_rows // 2
    local_heads = keys.shape[2] // HEAD_WIDTH
    group = queries.shape[2] // (local_heads * HEAD_WIDTH)
    width = group * HEAD_WIDTH
    deep = lax.axis_size("blk_0")
    swap = [(i, i ^ 1) for i in range(deep)]

    own_q = lax.dynamic_slice_in_dim(queries[0], half * width, width, 1)
    their_q = lax.ppermute(
        lax.dynamic_slice_in_dim(queries[0], (1 - half) * width, width, 1), "blk_0", swap
    )

    pieces = [keys[0, :, h * HEAD_WIDTH : (h + 1) * HEAD_WIDTH] for h in range(local_heads)]
    pieces += [values[0, :, h * HEAD_WIDTH : (h + 1) * HEAD_WIDTH] for h in range(local_heads)]
    packed = (jnp.stack(pieces).astype(jnp.float32) * SENT_SCALE).astype(jnp.float16)
    column = lax.all_gather(packed, "blk_0", axis=0, tiled=False)
    column = column.reshape(deep, 2, local_heads, tok_rows, HEAD_WIDTH)
    column = lax.dynamic_index_in_dim(column, half, 2, keepdims=False)
    gathered = lax.all_gather(column, "blk_1", axis=0, tiled=False).astype(jnp.bfloat16)

    spans = span_order.shape[0]
    every = jnp.arange(spans, dtype=jnp.int32)
    slot_of = jnp.sum(jnp.where(span_order[None, :] == every[:, None], every[None, :], 0), axis=1)

    def table_of(device):
        return jnp.concatenate(
            [slot_of, lax.dynamic_slice_in_dim(span_order, device * 2, 2), prompt_length]
        ).astype(jnp.int32)

    theirs = attend(table_of(partner), their_q, gathered, group, span)
    theirs, own_q = lax.optimization_barrier((theirs, own_q))
    other = lax.ppermute(theirs, "blk_0", swap)
    own = attend(table_of(mine), own_q, gathered, group, span)
    first = jnp.where(half == 0, own, other)
    second = jnp.where(half == 0, other, own)
    return jnp.concatenate([first, second], axis=1)[None]


def solution(mesh):
    blk = mesh.shape["blk"]
    split = Mesh(
        mesh.devices.reshape(mesh.shape["rep"], blk // 8, 8, mesh.shape["head"]),
        ("rep", "blk_0", "blk_1", "head"),
    )
    in_specs = (
        P("rep", BLK, "head"),
        P("rep", BLK, "head"),
        P("rep", BLK, "head"),
        P("rep"),
        P("rep"),
    )
    out_specs = P("rep", BLK, "head")
    return jax.shard_map(
        shards, mesh=split, in_specs=in_specs, out_specs=out_specs, check_vma=False
    )
```

```python
import jax
import jax.numpy as jnp
from jax import lax
from jax.experimental import pallas as pl
from jax.experimental.pallas import tpu as pltpu
from jax.sharding import Mesh
from jax.sharding import PartitionSpec as P

HEAD_WIDTH = 128
BLK = ("blk_0", "blk_1")
BLOCK_SPANS = 16
STEP_BLOCKS = 4
NEG_FILL = -1e30
LOG2_E = 1.4426950408889634
SENT_SCALE = 4096.0


def attend(table, q, gathered, group, span):
    spans = gathered.shape[0]
    blocks = spans // BLOCK_SPANS
    keys_of = BLOCK_SPANS * span
    rows = group * span
    factor = LOG2_E * HEAD_WIDTH ** (-0.5) / SENT_SCALE

    def kernel(table_ref, q_ref, kv_ref, o_ref, kept_ref, s_buf, q_buf, m_buf, acc_buf):
        limit = table_ref[spans + 2]

        def block(b, which):
            parts = [kv_ref[table_ref[b * BLOCK_SPANS + i], which] for i in range(BLOCK_SPANS)]
            return jnp.concatenate(parts, axis=0)

        def tile(which, _):
            place = table_ref[spans + which]
            count = jnp.where(place * span < limit, place // BLOCK_SPANS + 1, 0)
            row0 = pl.multiple_of(which * span, span)

            @pl.when(count == 0)
            def _():
                o_ref[pl.ds(row0, span), :] = jnp.zeros((span, group * HEAD_WIDTH), o_ref.dtype)

            @pl.when(count > 0)
            def _():
                for g in range(group):
                    q_buf[g * span : (g + 1) * span, :] = q_ref[
                        pl.ds(row0, span), g * HEAD_WIDTH : (g + 1) * HEAD_WIDTH
                    ]
                m_buf[...] = jnp.full(m_buf.shape, NEG_FILL, jnp.float32)
                acc_buf[...] = jnp.zeros(acc_buf.shape, jnp.float32)

                def score(first, size):
                    top = m_buf[...]
                    for u in range(size):
                        s = lax.dot_general(
                            q_buf[...],
                            block(first + u, 0),
                            (((1,), (1,)), ((), ())),
                            preferred_element_type=jnp.float32,
                        )
                        gap = place * span - (first + u) * keys_of
                        key = lax.broadcasted_iota(jnp.int32, (span, keys_of), 1)
                        row = lax.broadcasted_iota(jnp.int32, (span, keys_of), 0) + gap
                        s = jnp.where((key <= row)[None], s.reshape(group, span, keys_of), NEG_FILL)
                        s = s.reshape(rows, keys_of)
                        s_buf[first + u] = s
                        for c in range(keys_of // 128):
                            top = jnp.maximum(top, s[:, c * 128 : (c + 1) * 128])
                    m_buf[...] = top

                def mix(first, size):
                    top = jnp.concatenate([m_buf[...]] * (keys_of // 128), axis=1)
                    total = acc_buf[...]
                    for u in range(size):
                        w = jnp.exp2((s_buf[first + u] - top) * factor).astype(jnp.bfloat16)
                        v = block(first + u, 1)
                        wide = jnp.concatenate([v, jnp.ones_like(v)], axis=1)
                        total += jnp.dot(w, wide, preferred_element_type=jnp.float32)
                    acc_buf[...] = total

                whole = count // STEP_BLOCKS

                def score_step(i, _):
                    score(i * STEP_BLOCKS, STEP_BLOCKS)
                    return 0

                def score_last(b, _):
                    score(b, 1)
                    return 0

                lax.fori_loop(0, whole, score_step, 0)
                lax.fori_loop(whole * STEP_BLOCKS, count, score_last, 0)
                m_buf[...] = jnp.broadcast_to(jnp.max(m_buf[...], axis=1, keepdims=True), m_buf.shape)

                def mix_step(i, _):
                    mix(i * STEP_BLOCKS, STEP_BLOCKS)
                    return 0

                def mix_last(b, _):
                    mix(b, 1)
                    return 0

                lax.fori_loop(0, whole, mix_step, 0)
                lax.fori_loop(whole * STEP_BLOCKS, count, mix_last, 0)
                out = acc_buf[:, :HEAD_WIDTH] / (acc_buf[:, HEAD_WIDTH:] * SENT_SCALE)
                row_pos = place * span + lax.broadcasted_iota(jnp.int32, out.shape, 0) % span
                out = jnp.where(row_pos < limit, out, 0.0).astype(o_ref.dtype)
                for g in range(group):
                    o_ref[pl.ds(row0, span), g * HEAD_WIDTH : (g + 1) * HEAD_WIDTH] = out[
                        g * span : (g + 1) * span
                    ]

            return 0

        lax.fori_loop(0, 2, tile, 0)

    return pl.pallas_call(
        kernel,
        out_shape=(
            jax.ShapeDtypeStruct(q.shape, q.dtype),
            jax.ShapeDtypeStruct(gathered.shape, gathered.dtype),
        ),
        in_specs=[
            pl.BlockSpec(memory_space=pltpu.SMEM),
            pl.BlockSpec(memory_space=pltpu.VMEM),
            pl.BlockSpec(memory_space=pltpu.VMEM),
        ],
        out_specs=(pl.BlockSpec(memory_space=pltpu.VMEM), pl.BlockSpec(memory_space=pltpu.VMEM)),
        input_output_aliases={2: 1},
        scratch_shapes=[
            pltpu.VMEM((blocks, rows, keys_of), jnp.float32),
            pltpu.VMEM((rows, HEAD_WIDTH), jnp.bfloat16),
            pltpu.VMEM((rows, 128), jnp.float32),
            pltpu.VMEM((rows, 2 * HEAD_WIDTH), jnp.float32),
        ],
        compiler_params=pltpu.CompilerParams(vmem_limit_bytes=32 * 1024 * 1024),
    )(table, q, gathered)


def shards(queries, keys, values, prompt_length, span_order):
    mine = lax.axis_index(BLK)
    lines = lax.axis_size("blk_1")
    half = lax.axis_index("blk_0") % 2
    partner = mine + (1 - 2 * half) * lines
    tok_rows = queries.shape[1]
    span = tok_rows // 2
    local_heads = keys.shape[2] // HEAD_WIDTH
    group = queries.shape[2] // (local_heads * HEAD_WIDTH)
    width = group * HEAD_WIDTH
    deep = lax.axis_size("blk_0")
    swap = [(i, i ^ 1) for i in range(deep)]

    own_q = lax.dynamic_slice_in_dim(queries[0], half * width, width, 1)
    their_q = lax.ppermute(
        lax.dynamic_slice_in_dim(queries[0], (1 - half) * width, width, 1), "blk_0", swap
    )

    pieces = [
        jnp.stack([x[0, p * span : (p + 1) * span, h * HEAD_WIDTH : (h + 1) * HEAD_WIDTH] for x in (keys, values)])
        for h in range(local_heads)
        for p in range(2)
    ]
    packed = (jnp.stack(pieces).astype(jnp.float32) * SENT_SCALE).astype(jnp.float16)
    column = lax.all_gather(packed, "blk_0", axis=0, tiled=False)
    column = column.reshape(deep, local_heads, 2, 2, span, HEAD_WIDTH)
    column = lax.dynamic_index_in_dim(column, half, 1, keepdims=False)

    spans = span_order.shape[0]
    every = jnp.arange(spans, dtype=jnp.int32)
    held = ((every // 2) % lines * deep + every // (2 * lines)) * 2 + every % 2
    place_of = jnp.sum(jnp.where(span_order[None, :] == every[:, None], held[None, :], 0), axis=1)

    def table_of(device):
        return jnp.concatenate(
            [place_of, lax.dynamic_slice_in_dim(span_order, device * 2, 2), prompt_length]
        ).astype(jnp.int32)

    low = half == 0
    column, their_table, own_table, own_q, low = lax.optimization_barrier(
        (column, table_of(partner), table_of(mine), own_q, low)
    )
    gathered = lax.all_gather(column, "blk_1", axis=0, tiled=False).astype(jnp.bfloat16)
    gathered = gathered.reshape(spans, 2, span, HEAD_WIDTH)
    theirs, gathered = attend(their_table, their_q, gathered, group, span)
    other = lax.ppermute(theirs, "blk_0", swap)
    own, _ = attend(own_table, own_q, gathered, group, span)
    first = jnp.where(low, own, other)
    second = jnp.where(low, other, own)
    return jnp.concatenate([first, second], axis=1)[None]


def solution(mesh):
    blk = mesh.shape["blk"]
    split = Mesh(
        mesh.devices.reshape(mesh.shape["rep"], blk // 8, 8, mesh.shape["head"]),
        ("rep", "blk_0", "blk_1", "head"),
    )
    in_specs = (
        P("rep", BLK, "head"),
        P("rep", BLK, "head"),
        P("rep", BLK, "head"),
        P("rep"),
        P("rep"),
    )
    out_specs = P("rep", BLK, "head")
    return jax.shard_map(
        shards, mesh=split, in_specs=in_specs, out_specs=out_specs, check_vma=False
    )
```

```python
import jax
import jax.numpy as jnp
from jax import lax
from jax.experimental import pallas as pl
from jax.experimental.pallas import tpu as pltpu
from jax.sharding import Mesh
from jax.sharding import PartitionSpec as P

HEAD_WIDTH = 128
BLK = ("blk_0", "blk_1")
BLOCK_SPANS = 16
STEP_BLOCKS = (8, 4, 2, 1)
NEG_FILL = -1e30
LOG2_E = 1.4426950408889634
SENT_SCALE = 4096.0


def attend(span_order, prompt_length, q, gathered, group, span, away):
    spans = gathered.shape[0] // 2
    deep, lines = lax.axis_size("blk_0"), lax.axis_size("blk_1")
    blocks = spans // BLOCK_SPANS
    keys_of = BLOCK_SPANS * span
    rows = group * span
    factor = LOG2_E * HEAD_WIDTH ** (-0.5) / SENT_SCALE

    def kernel(order_ref, length_ref, q_ref, kv_ref, o_ref, kept_ref, held_ref, s_buf, q_buf, m_buf, acc_buf):
        limit = length_ref[0]
        depth = lax.axis_index("blk_0")
        if away:
            depth = depth + 1 - 2 * (depth % 2)
        device = depth * lines + lax.axis_index("blk_1")

        def note(i, _):
            for u in range(2 * lines):
                held_ref[order_ref[i * (2 * lines) + u]] = (u // 2 * deep + i) * 4 + u % 2
            return 0

        lax.fori_loop(0, deep, note, 0)

        def block(b, which):
            parts = [kv_ref[held_ref[b * BLOCK_SPANS + i] + 2 * which] for i in range(BLOCK_SPANS)]
            return jnp.concatenate(parts, axis=0)

        def tile(which, _):
            place = order_ref[2 * device + which]
            count = jnp.where(place * span < limit, place // BLOCK_SPANS + 1, 0)
            row0 = pl.multiple_of(which * span, span)

            @pl.when(count == 0)
            def _():
                o_ref[pl.ds(row0, span), :] = jnp.zeros((span, group * HEAD_WIDTH), o_ref.dtype)

            @pl.when(count > 0)
            def _():
                for g in range(group):
                    q_buf[g * span : (g + 1) * span, :] = q_ref[
                        pl.ds(row0, span), g * HEAD_WIDTH : (g + 1) * HEAD_WIDTH
                    ]
                m_buf[...] = jnp.full(m_buf.shape, NEG_FILL, jnp.float32)
                acc_buf[...] = jnp.zeros(acc_buf.shape, jnp.float32)

                def score(first, size):
                    top = m_buf[...]
                    for u in range(size):
                        s = lax.dot_general(
                            q_buf[...],
                            block(first + u, 0),
                            (((1,), (1,)), ((), ())),
                            preferred_element_type=jnp.float32,
                        )
                        gap = place * span - (first + u) * keys_of
                        key = lax.broadcasted_iota(jnp.int32, (span, keys_of), 1)
                        row = lax.broadcasted_iota(jnp.int32, (span, keys_of), 0) + gap
                        s = jnp.where((key <= row)[None], s.reshape(group, span, keys_of), NEG_FILL)
                        s = s.reshape(rows, keys_of)
                        s_buf[first + u] = s
                        for c in range(keys_of // 128):
                            top = jnp.maximum(top, s[:, c * 128 : (c + 1) * 128])
                    m_buf[...] = top

                def mix(first, size):
                    top = jnp.concatenate([m_buf[...]] * (keys_of // 128), axis=1)
                    total = acc_buf[...]
                    for u in range(size):
                        w = jnp.exp2((s_buf[first + u] - top) * factor).astype(jnp.bfloat16)
                        v = block(first + u, 1)
                        wide = jnp.concatenate([v, jnp.ones_like(v)], axis=1)
                        total += jnp.dot(w, wide, preferred_element_type=jnp.float32)
                    acc_buf[...] = total


                def in_steps(work):
                    done = 0
                    for size in STEP_BLOCKS:
                        times = (count - done) // size

                        def step(i, _, done=done, size=size):
                            work(done + i * size, size)
                            return 0

                        lax.fori_loop(0, times, step, 0)
                        done = done + times * size

                in_steps(score)
                m_buf[...] = jnp.broadcast_to(jnp.max(m_buf[...], axis=1, keepdims=True), m_buf.shape)
                in_steps(mix)
                out = acc_buf[:, :HEAD_WIDTH] / (acc_buf[:, HEAD_WIDTH:] * SENT_SCALE)
                row_pos = place * span + lax.broadcasted_iota(jnp.int32, out.shape, 0) % span
                out = jnp.where(row_pos < limit, out, 0.0).astype(o_ref.dtype)
                for g in range(group):
                    o_ref[pl.ds(row0, span), g * HEAD_WIDTH : (g + 1) * HEAD_WIDTH] = out[
                        g * span : (g + 1) * span
                    ]

            return 0

        lax.fori_loop(0, 2, tile, 0)

    return pl.pallas_call(
        kernel,
        out_shape=(
            jax.ShapeDtypeStruct(q.shape, q.dtype),
            jax.ShapeDtypeStruct(gathered.shape, gathered.dtype),
        ),
        in_specs=[
            pl.BlockSpec(memory_space=pltpu.SMEM),
            pl.BlockSpec(memory_space=pltpu.SMEM),
            pl.BlockSpec(memory_space=pltpu.VMEM),
            pl.BlockSpec(memory_space=pltpu.VMEM),
        ],
        out_specs=(pl.BlockSpec(memory_space=pltpu.VMEM), pl.BlockSpec(memory_space=pltpu.VMEM)),
        input_output_aliases={3: 1},
        scratch_shapes=[
            pltpu.SMEM((spans,), jnp.int32),
            pltpu.VMEM((blocks, rows, keys_of), jnp.float32),
            pltpu.VMEM((rows, HEAD_WIDTH), jnp.bfloat16),
            pltpu.VMEM((rows, 128), jnp.float32),
            pltpu.VMEM((rows, 2 * HEAD_WIDTH), jnp.float32),
        ],
        compiler_params=pltpu.CompilerParams(vmem_limit_bytes=32 * 1024 * 1024),
    )(span_order, prompt_length, q, gathered)


def shards(queries, keys, values, prompt_length, span_order):
    half = lax.axis_index("blk_0") % 2
    tok_rows = queries.shape[1]
    span = tok_rows // 2
    local_heads = keys.shape[2] // HEAD_WIDTH
    group = queries.shape[2] // (local_heads * HEAD_WIDTH)
    width = group * HEAD_WIDTH
    deep = lax.axis_size("blk_0")
    swap = [(i, i ^ 1) for i in range(deep)]

    own_q = lax.dynamic_slice_in_dim(queries[0], half * width, width, 1)
    their_q = lax.ppermute(
        lax.dynamic_slice_in_dim(queries[0], (1 - half) * width, width, 1), "blk_0", swap
    )

    pieces = [
        x[0, :, h * HEAD_WIDTH : (h + 1) * HEAD_WIDTH] for h in range(local_heads) for x in (keys, values)
    ]
    packed = (jnp.stack(pieces).astype(jnp.float32) * SENT_SCALE).astype(jnp.float16)
    column = lax.all_gather(packed, "blk_0", axis=0, tiled=False)
    column = column.reshape(deep, local_heads, 2, tok_rows, HEAD_WIDTH)
    column = lax.dynamic_index_in_dim(column, half, 1, keepdims=False)

    low = half == 0
    column, own_q, low = lax.optimization_barrier((column, own_q, low))
    gathered = lax.all_gather(column, "blk_1", axis=0, tiled=False).astype(jnp.bfloat16)
    gathered = gathered.reshape(-1, span, HEAD_WIDTH)
    theirs, gathered = attend(span_order, prompt_length, their_q, gathered, group, span, True)
    other = lax.ppermute(theirs, "blk_0", swap)
    own, _ = attend(span_order, prompt_length, own_q, gathered, group, span, False)
    first = jnp.where(low, own, other)
    second = jnp.where(low, other, own)
    return jnp.concatenate([first, second], axis=1)[None]


def solution(mesh):
    blk = mesh.shape["blk"]
    split = Mesh(
        mesh.devices.reshape(mesh.shape["rep"], blk // 8, 8, mesh.shape["head"]),
        ("rep", "blk_0", "blk_1", "head"),
    )
    in_specs = (
        P("rep", BLK, "head"),
        P("rep", BLK, "head"),
        P("rep", BLK, "head"),
        P("rep"),
        P("rep"),
    )
    out_specs = P("rep", BLK, "head")
    return jax.shard_map(
        shards, mesh=split, in_specs=in_specs, out_specs=out_specs, check_vma=False
    )
```

```python
import jax
import jax.numpy as jnp
from jax import lax
from jax.experimental import pallas as pl
from jax.experimental.pallas import tpu as pltpu
from jax.sharding import Mesh
from jax.sharding import PartitionSpec as P

HEAD_WIDTH = 128
BLK = ("blk_0", "blk_1")
BLOCK_SPANS = 16
STEP_BLOCKS = (8, 4, 2, 1)
NEG_FILL = -1e30
LOG2_E = 1.4426950408889634
SENT_SCALE = 4096.0


def attend(span_order, prompt_length, q, gathered, group, span, first, away):
    spans = gathered.shape[0] // 2
    deep, lines = lax.axis_size("blk_0"), lax.axis_size("blk_1")
    blocks = spans // BLOCK_SPANS
    keys_of = BLOCK_SPANS * span
    rows = group * span
    factor = LOG2_E * HEAD_WIDTH ** (-0.5) / SENT_SCALE

    def kernel(order_ref, length_ref, q_ref, kv_ref, o_ref, kept_ref, held_ref, s_buf, q_buf, m_buf, acc_buf):
        limit = length_ref[0]
        place_on = {name: lax.axis_index(name) for name in BLK}
        if away:
            place_on[first] = place_on[first] + 1 - 2 * (place_on[first] % 2)
        device = place_on["blk_0"] * lines + place_on["blk_1"]
        depth_step, line_step = (4, 4 * deep) if first == "blk_0" else (4 * lines, 4)

        def note(i, _):
            for u in range(2 * lines):
                held_ref[order_ref[i * (2 * lines) + u]] = u // 2 * line_step + i * depth_step + u % 2
            return 0

        lax.fori_loop(0, deep, note, 0)

        def block(b, which):
            parts = [kv_ref[held_ref[b * BLOCK_SPANS + i] + 2 * which] for i in range(BLOCK_SPANS)]
            return jnp.concatenate(parts, axis=0)

        def tile(which, _):
            place = order_ref[2 * device + which]
            count = jnp.where(place * span < limit, place // BLOCK_SPANS + 1, 0)
            row0 = pl.multiple_of(which * span, span)

            @pl.when(count == 0)
            def _():
                o_ref[pl.ds(row0, span), :] = jnp.zeros((span, group * HEAD_WIDTH), o_ref.dtype)

            @pl.when(count > 0)
            def _():
                for g in range(group):
                    q_buf[g * span : (g + 1) * span, :] = q_ref[
                        pl.ds(row0, span), g * HEAD_WIDTH : (g + 1) * HEAD_WIDTH
                    ]
                m_buf[...] = jnp.full(m_buf.shape, NEG_FILL, jnp.float32)
                acc_buf[...] = jnp.zeros(acc_buf.shape, jnp.float32)

                def score(first, size):
                    top = m_buf[...]
                    for u in range(size):
                        s = lax.dot_general(
                            q_buf[...],
                            block(first + u, 0),
                            (((1,), (1,)), ((), ())),
                            preferred_element_type=jnp.float32,
                        )
                        gap = place * span - (first + u) * keys_of
                        key = lax.broadcasted_iota(jnp.int32, (span, keys_of), 1)
                        row = lax.broadcasted_iota(jnp.int32, (span, keys_of), 0) + gap
                        s = jnp.where((key <= row)[None], s.reshape(group, span, keys_of), NEG_FILL)
                        s = s.reshape(rows, keys_of)
                        s_buf[first + u] = s
                        for c in range(keys_of // 128):
                            top = jnp.maximum(top, s[:, c * 128 : (c + 1) * 128])
                    m_buf[...] = top

                def mix(first, size):
                    top = jnp.concatenate([m_buf[...]] * (keys_of // 128), axis=1)
                    total = acc_buf[...]
                    for u in range(size):
                        w = jnp.exp2((s_buf[first + u] - top) * factor).astype(jnp.bfloat16)
                        v = block(first + u, 1)
                        wide = jnp.concatenate([v, jnp.ones_like(v)], axis=1)
                        total += jnp.dot(w, wide, preferred_element_type=jnp.float32)
                    acc_buf[...] = total


                def in_steps(work):
                    done = 0
                    for size in STEP_BLOCKS:
                        times = (count - done) // size

                        def step(i, _, done=done, size=size):
                            work(done + i * size, size)
                            return 0

                        lax.fori_loop(0, times, step, 0)
                        done = done + times * size

                in_steps(score)
                m_buf[...] = jnp.broadcast_to(jnp.max(m_buf[...], axis=1, keepdims=True), m_buf.shape)
                in_steps(mix)
                out = acc_buf[:, :HEAD_WIDTH] / (acc_buf[:, HEAD_WIDTH:] * SENT_SCALE)
                row_pos = place * span + lax.broadcasted_iota(jnp.int32, out.shape, 0) % span
                out = jnp.where(row_pos < limit, out, 0.0).astype(o_ref.dtype)
                for g in range(group):
                    o_ref[pl.ds(row0, span), g * HEAD_WIDTH : (g + 1) * HEAD_WIDTH] = out[
                        g * span : (g + 1) * span
                    ]

            return 0

        lax.fori_loop(0, 2, tile, 0)

    return pl.pallas_call(
        kernel,
        out_shape=(
            jax.ShapeDtypeStruct(q.shape, q.dtype),
            jax.ShapeDtypeStruct(gathered.shape, gathered.dtype),
        ),
        in_specs=[
            pl.BlockSpec(memory_space=pltpu.SMEM),
            pl.BlockSpec(memory_space=pltpu.SMEM),
            pl.BlockSpec(memory_space=pltpu.VMEM),
            pl.BlockSpec(memory_space=pltpu.VMEM),
        ],
        out_specs=(pl.BlockSpec(memory_space=pltpu.VMEM), pl.BlockSpec(memory_space=pltpu.VMEM)),
        input_output_aliases={3: 1},
        scratch_shapes=[
            pltpu.SMEM((spans,), jnp.int32),
            pltpu.VMEM((blocks, rows, keys_of), jnp.float32),
            pltpu.VMEM((rows, HEAD_WIDTH), jnp.bfloat16),
            pltpu.VMEM((rows, 128), jnp.float32),
            pltpu.VMEM((rows, 2 * HEAD_WIDTH), jnp.float32),
        ],
        compiler_params=pltpu.CompilerParams(vmem_limit_bytes=32 * 1024 * 1024),
    )(span_order, prompt_length, q, gathered)


def work(first, then):
    def run(queries, keys, values, prompt_length, span_order):
        half = lax.axis_index(first) % 2
        tok_rows = queries.shape[1]
        span = tok_rows // 2
        local_heads = keys.shape[2] // HEAD_WIDTH
        group = queries.shape[2] // (local_heads * HEAD_WIDTH)
        width = group * HEAD_WIDTH
        swap = [(i, i ^ 1) for i in range(lax.axis_size(first))]

        own_q = lax.dynamic_slice_in_dim(queries[0], half * width, width, 1)
        their_q = lax.ppermute(
            lax.dynamic_slice_in_dim(queries[0], (1 - half) * width, width, 1), first, swap
        )

        pieces = [
            x[0, :, h * HEAD_WIDTH : (h + 1) * HEAD_WIDTH] for h in range(local_heads) for x in (keys, values)
        ]
        packed = (jnp.stack(pieces).astype(jnp.float32) * SENT_SCALE).astype(jnp.float16)
        part = lax.all_gather(packed, first, axis=0, tiled=False)
        part = part.reshape(-1, local_heads, 2, tok_rows, HEAD_WIDTH)
        part = lax.dynamic_index_in_dim(part, half, 1, keepdims=False)

        low = half == 0
        part, own_q, low = lax.optimization_barrier((part, own_q, low))
        gathered = lax.all_gather(part, then, axis=0, tiled=False).astype(jnp.bfloat16)
        gathered = gathered.reshape(-1, span, HEAD_WIDTH)
        theirs, gathered = attend(span_order, prompt_length, their_q, gathered, group, span, first, True)
        other = lax.ppermute(theirs, first, swap)
        own, _ = attend(span_order, prompt_length, own_q, gathered, group, span, first, False)
        left = jnp.where(low, own, other)
        right = jnp.where(low, other, own)
        return jnp.concatenate([left, right], axis=1)[None]

    return run


def shards(queries, keys, values, prompt_length, span_order):
    return lax.cond(
        lax.axis_index("head") == 0,
        work("blk_0", "blk_1"),
        work("blk_1", "blk_0"),
        queries,
        keys,
        values,
        prompt_length,
        span_order,
    )


def solution(mesh):
    blk = mesh.shape["blk"]
    split = Mesh(
        mesh.devices.reshape(mesh.shape["rep"], blk // 8, 8, mesh.shape["head"]),
        ("rep", "blk_0", "blk_1", "head"),
    )
    in_specs = (
        P("rep", BLK, "head"),
        P("rep", BLK, "head"),
        P("rep", BLK, "head"),
        P("rep"),
        P("rep"),
    )
    out_specs = P("rep", BLK, "head")
    return jax.shard_map(
        shards, mesh=split, in_specs=in_specs, out_specs=out_specs, check_vma=False
    )
```

```python
import jax
import jax.numpy as jnp
from jax import lax
from jax.experimental import pallas as pl
from jax.experimental.pallas import tpu as pltpu
from jax.sharding import Mesh
from jax.sharding import PartitionSpec as P

HEAD_WIDTH = 128
BLK = ("blk_0", "blk_1")
BLOCK_SPANS = 16
STEP_BLOCKS = (8, 4, 2, 1)
NEG_FILL = -1e30
LOG2_E = 1.4426950408889634
SENT_SCALE = 4096.0


def attend(span_order, prompt_length, rows_of, gathered, partial, group, span, first):
    spans = gathered.shape[0] // 2
    deep, lines = lax.axis_size("blk_0"), lax.axis_size("blk_1")
    blocks = spans // BLOCK_SPANS
    opening = partial is None
    keys_of = BLOCK_SPANS * span
    rows = group * span
    factor = LOG2_E * HEAD_WIDTH ** (-0.5) / SENT_SCALE

    def kernel(order_ref, length_ref, *refs):
        if opening:
            their_q_ref, own_q_ref, kv_ref, their_o_ref, own_o_ref, kept_ref = refs[:6]
        else:
            own_q_ref, kv_ref, partial_ref, own_o_ref, kept_ref = refs[:5]
        held_ref, s_buf, q_buf, m_buf, acc_buf, o_buf = refs[-6:]
        limit = length_ref[0]
        place_on = {name: lax.axis_index(name) for name in BLK}
        own_device = place_on["blk_0"] * lines + place_on["blk_1"]
        place_on[first] = place_on[first] + 1 - 2 * (place_on[first] % 2)
        their_device = place_on["blk_0"] * lines + place_on["blk_1"]

        def blocks_for(device, which):
            place = order_ref[2 * device + which]
            return jnp.where(place * span < limit, place // BLOCK_SPANS + 1, 0)

        costs = [blocks_for(own_device, 0), blocks_for(own_device, 1)]
        ahead = costs[0] + costs[1] - blocks_for(their_device, 0) - blocks_for(their_device, 1)
        early = jnp.where(jnp.abs(costs[1] - ahead) < jnp.abs(costs[0] - ahead), 1, 0)
        gain = jnp.abs(jnp.where(early == 1, costs[1], costs[0]) - ahead) < ahead
        depth_step, line_step = (4, 4 * deep) if first == "blk_0" else (4 * lines, 4)

        def note(i, _):
            for u in range(2 * lines):
                held_ref[order_ref[i * (2 * lines) + u]] = u // 2 * line_step + i * depth_step + u % 2
            return 0

        lax.fori_loop(0, deep, note, 0)

        def block(b, which):
            parts = [kv_ref[held_ref[b * BLOCK_SPANS + i] + 2 * which] for i in range(BLOCK_SPANS)]
            return jnp.concatenate(parts, axis=0)

        def tile(t, _):
            if opening:
                theirs = t < 2
                which = jnp.where(theirs, t, early)
                device = jnp.where(theirs, their_device, own_device)
            else:
                theirs = None
                which = t
                device = own_device
            place = order_ref[2 * device + which]
            count = jnp.where(place * span < limit, place // BLOCK_SPANS + 1, 0)
            row0 = pl.multiple_of(which * span, span)

            def load(q_ref):
                for g in range(group):
                    q_buf[g * span : (g + 1) * span, :] = q_ref[
                        pl.ds(row0, span), g * HEAD_WIDTH : (g + 1) * HEAD_WIDTH
                    ]

            def store(o_ref):
                o_ref[pl.ds(row0, span), :] = o_buf[...]

            @pl.when(count == 0)
            def _():
                o_buf[...] = jnp.zeros(o_buf.shape, o_buf.dtype)

            @pl.when(count > 0)
            def _():
                if opening:
                    pl.when(theirs)(lambda: load(their_q_ref))
                    pl.when(jnp.logical_not(theirs))(lambda: load(own_q_ref))
                else:
                    load(own_q_ref)
                m_buf[...] = jnp.full(m_buf.shape, NEG_FILL, jnp.float32)
                acc_buf[...] = jnp.zeros(acc_buf.shape, jnp.float32)

                def score(first, size):
                    top = m_buf[...]
                    for u in range(size):
                        s = lax.dot_general(
                            q_buf[...],
                            block(first + u, 0),
                            (((1,), (1,)), ((), ())),
                            preferred_element_type=jnp.float32,
                        )
                        gap = place * span - (first + u) * keys_of
                        key = lax.broadcasted_iota(jnp.int32, (span, keys_of), 1)
                        row = lax.broadcasted_iota(jnp.int32, (span, keys_of), 0) + gap
                        s = jnp.where((key <= row)[None], s.reshape(group, span, keys_of), NEG_FILL)
                        s = s.reshape(rows, keys_of)
                        s_buf[first + u] = s
                        for c in range(keys_of // 128):
                            top = jnp.maximum(top, s[:, c * 128 : (c + 1) * 128])
                    m_buf[...] = top

                def mix(first, size):
                    top = jnp.concatenate([m_buf[...]] * (keys_of // 128), axis=1)
                    total = acc_buf[...]
                    for u in range(size):
                        w = jnp.exp2((s_buf[first + u] - top) * factor).astype(jnp.bfloat16)
                        v = block(first + u, 1)
                        wide = jnp.concatenate([v, jnp.ones_like(v)], axis=1)
                        total += jnp.dot(w, wide, preferred_element_type=jnp.float32)
                    acc_buf[...] = total


                def in_steps(work):
                    done = 0
                    for size in STEP_BLOCKS:
                        times = (count - done) // size

                        def step(i, _, done=done, size=size):
                            work(done + i * size, size)
                            return 0

                        lax.fori_loop(0, times, step, 0)
                        done = done + times * size

                in_steps(score)
                m_buf[...] = jnp.broadcast_to(jnp.max(m_buf[...], axis=1, keepdims=True), m_buf.shape)
                in_steps(mix)
                out = acc_buf[:, :HEAD_WIDTH] / (acc_buf[:, HEAD_WIDTH:] * SENT_SCALE)
                row_pos = place * span + lax.broadcasted_iota(jnp.int32, out.shape, 0) % span
                out = jnp.where(row_pos < limit, out, 0.0).astype(o_buf.dtype)
                for g in range(group):
                    o_buf[:, g * HEAD_WIDTH : (g + 1) * HEAD_WIDTH] = out[g * span : (g + 1) * span]

            if opening:
                pl.when(theirs)(lambda: store(their_o_ref))
                pl.when(jnp.logical_not(theirs))(lambda: store(own_o_ref))
            else:
                store(own_o_ref)
            return 0

        if opening:
            lax.fori_loop(0, jnp.where(gain, 3, 2), tile, 0)
        else:
            begin = jnp.where(gain & (early == 0), 1, 0)
            lax.fori_loop(begin, jnp.where(gain & (early == 1), 1, 2), tile, 0)

    vmem = pl.BlockSpec(memory_space=pltpu.VMEM)
    smem = pl.BlockSpec(memory_space=pltpu.SMEM)
    rows_shape = jax.ShapeDtypeStruct(rows_of[0].shape, rows_of[0].dtype)
    operands = [*rows_of, gathered] + ([] if opening else [partial])
    outs = len(rows_of) + 1
    return pl.pallas_call(
        kernel,
        out_shape=(rows_shape,) * len(rows_of) + (jax.ShapeDtypeStruct(gathered.shape, gathered.dtype),),
        in_specs=[smem, smem] + [vmem] * len(operands),
        out_specs=(vmem,) * outs,
        input_output_aliases={4: 2} if opening else {3: 1, 4: 0},
        scratch_shapes=[
            pltpu.SMEM((spans,), jnp.int32),
            pltpu.VMEM((blocks, rows, keys_of), jnp.float32),
            pltpu.VMEM((rows, HEAD_WIDTH), jnp.bfloat16),
            pltpu.VMEM((rows, 128), jnp.float32),
            pltpu.VMEM((rows, 2 * HEAD_WIDTH), jnp.float32),
            pltpu.VMEM((span, group * HEAD_WIDTH), jnp.bfloat16),
        ],
        compiler_params=pltpu.CompilerParams(vmem_limit_bytes=32 * 1024 * 1024),
    )(span_order, prompt_length, *operands)


def work(first, then):
    def run(queries, keys, values, prompt_length, span_order):
        half = lax.axis_index(first) % 2
        tok_rows = queries.shape[1]
        span = tok_rows // 2
        local_heads = keys.shape[2] // HEAD_WIDTH
        group = queries.shape[2] // (local_heads * HEAD_WIDTH)
        width = group * HEAD_WIDTH
        swap = [(i, i ^ 1) for i in range(lax.axis_size(first))]

        own_q = lax.dynamic_slice_in_dim(queries[0], half * width, width, 1)
        their_q = lax.ppermute(
            lax.dynamic_slice_in_dim(queries[0], (1 - half) * width, width, 1), first, swap
        )

        pieces = [
            x[0, :, h * HEAD_WIDTH : (h + 1) * HEAD_WIDTH] for h in range(local_heads) for x in (keys, values)
        ]
        packed = (jnp.stack(pieces).astype(jnp.float32) * SENT_SCALE).astype(jnp.float16)
        part = lax.all_gather(packed, first, axis=0, tiled=False)
        part = part.reshape(-1, local_heads, 2, tok_rows, HEAD_WIDTH)
        part = lax.dynamic_index_in_dim(part, half, 1, keepdims=False)

        low = half == 0
        part, own_q, low = lax.optimization_barrier((part, own_q, low))
        gathered = lax.all_gather(part, then, axis=0, tiled=False).astype(jnp.bfloat16)
        gathered = gathered.reshape(-1, span, HEAD_WIDTH)
        theirs, own, gathered = attend(
            span_order, prompt_length, (their_q, own_q), gathered, None, group, span, first
        )
        other = lax.ppermute(theirs, first, swap)
        own, _ = attend(span_order, prompt_length, (own_q,), gathered, own, group, span, first)
        left = jnp.where(low, own, other)
        right = jnp.where(low, other, own)
        return jnp.concatenate([left, right], axis=1)[None]

    return run


def shards(queries, keys, values, prompt_length, span_order):
    return lax.cond(
        lax.axis_index("head") == 0,
        work("blk_0", "blk_1"),
        work("blk_1", "blk_0"),
        queries,
        keys,
        values,
        prompt_length,
        span_order,
    )


def solution(mesh):
    blk = mesh.shape["blk"]
    split = Mesh(
        mesh.devices.reshape(mesh.shape["rep"], blk // 8, 8, mesh.shape["head"]),
        ("rep", "blk_0", "blk_1", "head"),
    )
    in_specs = (
        P("rep", BLK, "head"),
        P("rep", BLK, "head"),
        P("rep", BLK, "head"),
        P("rep"),
        P("rep"),
    )
    out_specs = P("rep", BLK, "head")
    return jax.shard_map(
        shards, mesh=split, in_specs=in_specs, out_specs=out_specs, check_vma=False
    )
```

```python
import jax
import jax.numpy as jnp
from jax import lax
from jax.experimental import pallas as pl
from jax.experimental.pallas import tpu as pltpu
from jax.sharding import Mesh
from jax.sharding import PartitionSpec as P

HEAD_WIDTH = 128
BLK = ("blk_0", "blk_1")
BLOCK_SPANS = 8
STEP_BLOCKS = (16, 8, 4, 2, 1)
NEG_FILL = -1e30
LOG2_E = 1.4426950408889634
SENT_SCALE = 4096.0


def attend(span_order, prompt_length, rows_of, gathered, partial, group, span, first):
    spans = gathered.shape[0] // 2
    deep, lines = lax.axis_size("blk_0"), lax.axis_size("blk_1")
    blocks = spans // BLOCK_SPANS
    opening = partial is None
    keys_of = BLOCK_SPANS * span
    rows = group * span
    factor = LOG2_E * HEAD_WIDTH ** (-0.5) / SENT_SCALE

    def kernel(order_ref, length_ref, *refs):
        if opening:
            their_q_ref, own_q_ref, kv_ref, their_o_ref, own_o_ref, kept_ref = refs[:6]
        else:
            own_q_ref, kv_ref, partial_ref, own_o_ref, kept_ref = refs[:5]
        held_ref, s_buf, q_buf, m_buf, acc_buf, o_buf = refs[-6:]
        limit = length_ref[0]
        place_on = {name: lax.axis_index(name) for name in BLK}
        own_device = place_on["blk_0"] * lines + place_on["blk_1"]
        place_on[first] = place_on[first] + 1 - 2 * (place_on[first] % 2)
        their_device = place_on["blk_0"] * lines + place_on["blk_1"]

        def blocks_for(device, which):
            place = order_ref[2 * device + which]
            return jnp.where(place * span < limit, place // BLOCK_SPANS + 1, 0)

        costs = [blocks_for(own_device, 0), blocks_for(own_device, 1)]
        ahead = costs[0] + costs[1] - blocks_for(their_device, 0) - blocks_for(their_device, 1)
        early = jnp.where(jnp.abs(costs[1] - ahead) < jnp.abs(costs[0] - ahead), 1, 0)
        gain = jnp.abs(jnp.where(early == 1, costs[1], costs[0]) - ahead) < ahead
        depth_step, line_step = (4, 4 * deep) if first == "blk_0" else (4 * lines, 4)

        def note(i, _):
            for u in range(2 * lines):
                held_ref[order_ref[i * (2 * lines) + u]] = u // 2 * line_step + i * depth_step + u % 2
            return 0

        lax.fori_loop(0, deep, note, 0)

        def block(b, which):
            parts = [kv_ref[held_ref[b * BLOCK_SPANS + i] + 2 * which] for i in range(BLOCK_SPANS)]
            return jnp.concatenate(parts, axis=0)

        def tile(t, _):
            if opening:
                theirs = t < 2
                which = jnp.where(theirs, t, early)
                device = jnp.where(theirs, their_device, own_device)
            else:
                theirs = None
                which = t
                device = own_device
            place = order_ref[2 * device + which]
            count = jnp.where(place * span < limit, place // BLOCK_SPANS + 1, 0)
            row0 = pl.multiple_of(which * span, span)

            def load(q_ref):
                for g in range(group):
                    q_buf[g * span : (g + 1) * span, :] = q_ref[
                        pl.ds(row0, span), g * HEAD_WIDTH : (g + 1) * HEAD_WIDTH
                    ]

            def store(o_ref):
                o_ref[pl.ds(row0, span), :] = o_buf[...]

            @pl.when(count == 0)
            def _():
                o_buf[...] = jnp.zeros(o_buf.shape, o_buf.dtype)

            @pl.when(count > 0)
            def _():
                if opening:
                    pl.when(theirs)(lambda: load(their_q_ref))
                    pl.when(jnp.logical_not(theirs))(lambda: load(own_q_ref))
                else:
                    load(own_q_ref)
                m_buf[...] = jnp.full(m_buf.shape, NEG_FILL, jnp.float32)
                acc_buf[...] = jnp.zeros(acc_buf.shape, jnp.float32)

                def score(first, size):
                    top = m_buf[...]
                    for u in range(size):
                        s = lax.dot_general(
                            q_buf[...],
                            block(first + u, 0),
                            (((1,), (1,)), ((), ())),
                            preferred_element_type=jnp.float32,
                        )
                        gap = place * span - (first + u) * keys_of
                        key = lax.broadcasted_iota(jnp.int32, (span, keys_of), 1)
                        row = lax.broadcasted_iota(jnp.int32, (span, keys_of), 0) + gap
                        s = jnp.where((key <= row)[None], s.reshape(group, span, keys_of), NEG_FILL)
                        s = s.reshape(rows, keys_of)
                        s_buf[first + u] = s
                        for c in range(keys_of // 128):
                            top = jnp.maximum(top, s[:, c * 128 : (c + 1) * 128])
                    m_buf[...] = top

                def mix(first, size):
                    top = jnp.concatenate([m_buf[...]] * (keys_of // 128), axis=1)
                    total = acc_buf[...]
                    for u in range(size):
                        w = jnp.exp2((s_buf[first + u] - top) * factor).astype(jnp.bfloat16)
                        v = block(first + u, 1)
                        wide = jnp.concatenate([v, jnp.ones_like(v)], axis=1)
                        total += jnp.dot(w, wide, preferred_element_type=jnp.float32)
                    acc_buf[...] = total


                def in_steps(work):
                    done = 0
                    for size in STEP_BLOCKS:
                        times = (count - done) // size

                        def step(i, _, done=done, size=size):
                            work(done + i * size, size)
                            return 0

                        lax.fori_loop(0, times, step, 0)
                        done = done + times * size

                in_steps(score)
                m_buf[...] = jnp.broadcast_to(jnp.max(m_buf[...], axis=1, keepdims=True), m_buf.shape)
                in_steps(mix)
                out = acc_buf[:, :HEAD_WIDTH] / (acc_buf[:, HEAD_WIDTH:] * SENT_SCALE)
                row_pos = place * span + lax.broadcasted_iota(jnp.int32, out.shape, 0) % span
                out = jnp.where(row_pos < limit, out, 0.0).astype(o_buf.dtype)
                for g in range(group):
                    o_buf[:, g * HEAD_WIDTH : (g + 1) * HEAD_WIDTH] = out[g * span : (g + 1) * span]

            if opening:
                pl.when(theirs)(lambda: store(their_o_ref))
                pl.when(jnp.logical_not(theirs))(lambda: store(own_o_ref))
            else:
                store(own_o_ref)
            return 0

        if opening:
            lax.fori_loop(0, jnp.where(gain, 3, 2), tile, 0)
        else:
            begin = jnp.where(gain & (early == 0), 1, 0)
            lax.fori_loop(begin, jnp.where(gain & (early == 1), 1, 2), tile, 0)

    vmem = pl.BlockSpec(memory_space=pltpu.VMEM)
    smem = pl.BlockSpec(memory_space=pltpu.SMEM)
    rows_shape = jax.ShapeDtypeStruct(rows_of[0].shape, rows_of[0].dtype)
    operands = [*rows_of, gathered] + ([] if opening else [partial])
    outs = len(rows_of) + 1
    return pl.pallas_call(
        kernel,
        out_shape=(rows_shape,) * len(rows_of) + (jax.ShapeDtypeStruct(gathered.shape, gathered.dtype),),
        in_specs=[smem, smem] + [vmem] * len(operands),
        out_specs=(vmem,) * outs,
        input_output_aliases={4: 2} if opening else {3: 1, 4: 0},
        scratch_shapes=[
            pltpu.SMEM((spans,), jnp.int32),
            pltpu.VMEM((blocks, rows, keys_of), jnp.float32),
            pltpu.VMEM((rows, HEAD_WIDTH), jnp.bfloat16),
            pltpu.VMEM((rows, 128), jnp.float32),
            pltpu.VMEM((rows, 2 * HEAD_WIDTH), jnp.float32),
            pltpu.VMEM((span, group * HEAD_WIDTH), jnp.bfloat16),
        ],
        compiler_params=pltpu.CompilerParams(vmem_limit_bytes=32 * 1024 * 1024),
    )(span_order, prompt_length, *operands)


def work(first, then):
    def run(queries, keys, values, prompt_length, span_order):
        half = lax.axis_index(first) % 2
        tok_rows = queries.shape[1]
        span = tok_rows // 2
        local_heads = keys.shape[2] // HEAD_WIDTH
        group = queries.shape[2] // (local_heads * HEAD_WIDTH)
        width = group * HEAD_WIDTH
        swap = [(i, i ^ 1) for i in range(lax.axis_size(first))]

        own_q = lax.dynamic_slice_in_dim(queries[0], half * width, width, 1)
        their_q = lax.ppermute(
            lax.dynamic_slice_in_dim(queries[0], (1 - half) * width, width, 1), first, swap
        )

        pieces = [
            x[0, :, h * HEAD_WIDTH : (h + 1) * HEAD_WIDTH] for h in range(local_heads) for x in (keys, values)
        ]
        packed = (jnp.stack(pieces).astype(jnp.float32) * SENT_SCALE).astype(jnp.float16)
        part = lax.all_gather(packed, first, axis=0, tiled=False)
        part = part.reshape(-1, local_heads, 2, tok_rows, HEAD_WIDTH)
        part = lax.dynamic_index_in_dim(part, half, 1, keepdims=False)

        low = half == 0
        part, own_q, low = lax.optimization_barrier((part, own_q, low))
        gathered = lax.all_gather(part, then, axis=0, tiled=False).astype(jnp.bfloat16)
        gathered = gathered.reshape(-1, span, HEAD_WIDTH)
        theirs, own, gathered = attend(
            span_order, prompt_length, (their_q, own_q), gathered, None, group, span, first
        )
        other = lax.ppermute(theirs, first, swap)
        own, _ = attend(span_order, prompt_length, (own_q,), gathered, own, group, span, first)
        left = jnp.where(low, own, other)
        right = jnp.where(low, other, own)
        return jnp.concatenate([left, right], axis=1)[None]

    return run


def shards(queries, keys, values, prompt_length, span_order):
    return lax.cond(
        lax.axis_index("head") == 0,
        work("blk_0", "blk_1"),
        work("blk_1", "blk_0"),
        queries,
        keys,
        values,
        prompt_length,
        span_order,
    )


def solution(mesh):
    blk = mesh.shape["blk"]
    split = Mesh(
        mesh.devices.reshape(mesh.shape["rep"], blk // 8, 8, mesh.shape["head"]),
        ("rep", "blk_0", "blk_1", "head"),
    )
    in_specs = (
        P("rep", BLK, "head"),
        P("rep", BLK, "head"),
        P("rep", BLK, "head"),
        P("rep"),
        P("rep"),
    )
    out_specs = P("rep", BLK, "head")
    return jax.shard_map(
        shards, mesh=split, in_specs=in_specs, out_specs=out_specs, check_vma=False
    )
```
